8 devices in a mesh: dp: 1 (over z), tp: 2 (over y), cp: 4 (over x, core).
Axes of the slice: x: 2, y: 2, z: 1, core: 2. Of those that a mesh axis runs over, the one named last changes fastest.
Arguments:
- x_in: bfloat16 [4096, 8192], P(('dp', 'cp', 'tp'))
- seg_ids: int32 [4096], P(('dp', 'cp', 'tp'))
- w_q: bfloat16 [8192, 64, 128], P(None, 'tp')
- w_k: bfloat16 [8192, 64, 128], P(None, 'tp')
- w_v: bfloat16 [8192, 64, 128], P(None, 'tp')
- w_o: bfloat16 [64, 128, 8192], P('tp')
Outputs:
- output: bfloat16 [4096, 8192], P(('dp', 'cp', 'tp'))
All inputs are finite; a program needn't handle non-finite values.
Results may differ from the reference program's by a relative error of at most 0.00426498.
Values are sent between devices in bfloat16 or wider.
A program may use at most 1.25 GiB of HBM per device.

```python
import jax
import jax.numpy as jnp
from jax import lax

CP = 4
PIECE = 512
D = 8192
HEADS = 64
KV_HEADS = 64
HEAD = 128
DOCS = 6
QROWS = 64
SEQ = 2 * CP * PIECE
GROUP = HEADS // KV_HEADS


def row_positions():
    row_idx = jnp.arange(SEQ)
    owner_rank = row_idx // (2 * PIECE)
    within = row_idx % (2 * PIECE)
    return jnp.where(within < PIECE, owner_rank * PIECE + within, (2 * CP - 1 - owner_rank) * PIECE + within - PIECE)


def draw_segments(seg_key):
    half_len = SEQ // 2
    key_cut, key_gap = jax.random.split(seg_key)
    offsets = jax.random.permutation(key_cut, half_len - 1)[: DOCS - 1] + 1
    gap_start = jax.random.randint(key_gap, (), 0, half_len)
    cut_points = offsets + half_len * (offsets > gap_start).astype(jnp.int32)
    seq_pos = jnp.arange(SEQ)
    seg_seq = jnp.sum((seq_pos[:, None] >= cut_points[None, :]).astype(jnp.int32), axis=1)
    return seg_seq[row_positions()].astype(jnp.int32)


def setup_inputs(seed: int = 0, part: int = 0) -> dict:
    part_key = jax.random.fold_in(jax.random.key(seed), part)
    key_x, key_seg = jax.random.split(part_key)
    key_q, key_k, key_v, key_o = jax.random.split(jax.random.key(seed + 1), 4)
    x_in = jax.random.normal(key_x, (SEQ, D), jnp.float32).astype(jnp.bfloat16)
    seg_ids = draw_segments(key_seg)
    w_q = (jax.random.normal(key_q, (D, HEADS, HEAD), jnp.float32) * (1.5 * D ** -0.5)).astype(jnp.bfloat16)
    w_k = (jax.random.normal(key_k, (D, KV_HEADS, HEAD), jnp.float32) * D ** -0.5).astype(jnp.bfloat16)
    w_v = (jax.random.normal(key_v, (D, KV_HEADS, HEAD), jnp.float32) * D ** -0.5).astype(jnp.bfloat16)
    w_o = (jax.random.normal(key_o, (HEADS, HEAD, D), jnp.float32) * (4.0 * (HEADS * HEAD) ** -0.5)).astype(jnp.bfloat16)
    return {"x_in": x_in, "seg_ids": seg_ids, "w_q": w_q, "w_k": w_k, "w_v": w_v, "w_o": w_o}


def reference(x_in, seg_ids, w_q, w_k, w_v, w_o):
    pos_rows = row_positions()
    q_rows = jnp.dot(x_in, w_q.reshape(D, HEADS * HEAD), preferred_element_type=jnp.float32).astype(jnp.bfloat16)
    k_rows = jnp.dot(x_in, w_k.reshape(D, KV_HEADS * HEAD), preferred_element_type=jnp.float32).astype(jnp.bfloat16)
    v_rows = jnp.dot(x_in, w_v.reshape(D, KV_HEADS * HEAD), preferred_element_type=jnp.float32).astype(jnp.bfloat16)
    q_blocks = q_rows.reshape(SEQ // QROWS, QROWS, KV_HEADS, GROUP, HEAD).astype(jnp.float32)
    k_heads = k_rows.reshape(SEQ, KV_HEADS, HEAD).transpose(1, 0, 2).astype(jnp.float32)
    v_heads = v_rows.reshape(SEQ, KV_HEADS, HEAD).transpose(1, 0, 2).astype(jnp.float32)
    pos_blocks = pos_rows.reshape(SEQ // QROWS, QROWS)
    seg_blocks = seg_ids.reshape(SEQ // QROWS, QROWS)

    def query_block(blk_args):
        q_blk, pos_blk, seg_blk = blk_args
        visible = (seg_blk[:, None] == seg_ids[None, :]) & (pos_rows[None, :] <= pos_blk[:, None])

        def kv_head(head_args):
            q_head, k_head, v_head = head_args
            scores = jnp.einsum("qge,se->gqs", q_head, k_head) * HEAD ** -0.5
            scores = jnp.where(visible[None], scores, -jnp.inf)
            prob_rows = jnp.exp(scores - jnp.max(scores, axis=-1, keepdims=True))
            row_sum = jnp.sum(prob_rows, axis=-1)
            pv_sum = jnp.einsum("gqs,se->gqe", prob_rows.astype(jnp.bfloat16).astype(jnp.float32), v_head)
            return (pv_sum / row_sum[..., None]).astype(jnp.bfloat16)

        return lax.map(kv_head, (q_blk.transpose(1, 0, 2, 3), k_heads, v_heads))

    attn_rows = lax.map(query_block, (q_blocks, pos_blocks, seg_blocks))
    attn_rows = attn_rows.transpose(0, 3, 1, 2, 4).reshape(SEQ, HEADS * HEAD)
    y_out = jnp.dot(attn_rows, w_o.reshape(HEADS * HEAD, D), preferred_element_type=jnp.float32)
    return y_out.astype(jnp.bfloat16)
```

```python
import functools
import math

import jax
import jax.numpy as jnp
from jax import lax
from jax.experimental import pallas as pl
from jax.experimental.pallas import tpu as pltpu
from jax.sharding import PartitionSpec as P


NEG_BIG = -1e30
N_CP = 4
PIECE = 512
X_CHUNKS = 2
Y_SPLITS = (512, 1024, 1024, 1024, 1024, 1024, 1024, 1024, 512)
SWAP = [(0, 1), (1, 0)]


def attn_kernel(meta_ref, start_ref, *refs, n_heads, chunk_rows, q_chunks, coef):
    n_parts = len(chunk_rows)
    n_k = N_CP * n_parts
    n_q = N_CP * len(q_chunks)
    k_refs, v_refs = refs[:n_k], refs[n_k:2 * n_k]
    q_refs = refs[2 * n_k:2 * n_k + n_q]
    o_ref = refs[2 * n_k + n_q]
    k_buf, v_buf, q_buf, m_ref, l_ref, acc_ref, sems = refs[2 * n_k + n_q + 1:]
    head = pl.program_id(0)

    def copies(head_idx, slot):
        out = []
        for src in range(N_CP):
            for part, (kind, row0, rows) in enumerate(chunk_rows):
                piece = meta_ref[kind * N_CP + src]
                dst = pl.ds(pl.multiple_of(piece * PIECE + row0, 128), rows)
                idx = src * n_parts + part
                out.append(pltpu.make_async_copy(k_refs[idx].at[head_idx], k_buf.at[slot, dst], sems.at[slot]))
                out.append(pltpu.make_async_copy(v_refs[idx].at[head_idx], v_buf.at[slot, dst], sems.at[slot]))
            for part, (row0, rows) in enumerate(q_chunks):
                idx = src * len(q_chunks) + part
                out.append(pltpu.make_async_copy(q_refs[idx].at[head_idx], q_buf.at[slot, src, pl.ds(row0, rows)], sems.at[slot]))
        return out

    slot = lax.rem(head, 2)

    @pl.when(head == 0)
    def _():
        for cp in copies(0, 0):
            cp.start()

    @pl.when(head + 1 < n_heads)
    def _():
        for cp in copies(head + 1, 1 - slot):
            cp.start()

    for cp in copies(head, slot):
        cp.wait()

    row_i = lax.broadcasted_iota(jnp.int32, (PIECE, PIECE), 0)
    col_i = lax.broadcasted_iota(jnp.int32, (PIECE, PIECE), 1)

    for src in range(N_CP):
        q_piece = meta_ref[2 * N_CP + src]
        k_lo = meta_ref[3 * N_CP + q_piece]
        k_full = meta_ref[3 * N_CP + 2 * N_CP + q_piece]
        q0 = pl.multiple_of(q_piece * PIECE, PIECE)
        q_blk = q_buf[slot, src]
        starts = start_ref[pl.ds(q0, PIECE), :]

        def scores_of(k0):
            return lax.dot_general(q_blk, k_buf[slot, pl.ds(k0, PIECE), :], (((1,), (1,)), ((), ())), preferred_element_type=jnp.float32)

        def fold(p):
            total = p[:, :128]
            for lane in range(128, PIECE, 128):
                total = total + p[:, lane:lane + 128]
            return total

        s = scores_of(q0)
        s = jnp.where((col_i <= row_i) & (col_i >= starts - q0), s, NEG_BIG)
        m_new = jnp.max(s, axis=1, keepdims=True)
        p = jnp.exp2(s * coef - m_new * coef)
        m_ref[...] = jnp.broadcast_to(m_new, m_ref.shape)
        l_ref[...] = fold(p)
        acc_ref[...] = jnp.dot(p.astype(jnp.bfloat16), v_buf[slot, pl.ds(q0, PIECE), :], preferred_element_type=jnp.float32)

        def step(kb, masked):
            k0 = pl.multiple_of(kb * PIECE, PIECE)
            s = scores_of(k0)
            if masked:
                s = jnp.where(col_i >= starts - k0, s, NEG_BIG)
            m_old = m_ref[:, :1]
            m_new = jnp.maximum(m_old, jnp.max(s, axis=1, keepdims=True))
            alpha = jnp.exp2((m_old - m_new) * coef)
            p = jnp.exp2(s * coef - m_new * coef)
            m_ref[...] = jnp.broadcast_to(m_new, m_ref.shape)
            l_ref[...] = l_ref[...] * alpha + fold(p)
            acc_ref[...] = acc_ref[...] * alpha + jnp.dot(p.astype(jnp.bfloat16), v_buf[slot, pl.ds(k0, PIECE), :], preferred_element_type=jnp.float32)

        pl.loop(k_lo, k_full)(lambda kb: step(kb, True))
        pl.loop(k_full, q_piece)(lambda kb: step(kb, False))
        total = jnp.sum(l_ref[...], axis=1, keepdims=True)
        o_ref[src] = (acc_ref[...] / total).astype(jnp.bfloat16)


def attention(meta, starts, k_parts, v_parts, q_parts, chunk_rows, q_chunks, coef):
    n_heads, _, head_dim = k_parts[0].shape
    n_in = len(k_parts) + len(v_parts) + len(q_parts)
    seq = starts.shape[0]
    return pl.pallas_call(
        functools.partial(attn_kernel, n_heads=n_heads, chunk_rows=chunk_rows, q_chunks=q_chunks, coef=coef),
        grid_spec=pltpu.PrefetchScalarGridSpec(
            num_scalar_prefetch=1,
            grid=(n_heads,),
            in_specs=[pl.BlockSpec((seq, 1), lambda h, meta: (0, 0))] + [pl.BlockSpec(memory_space=pltpu.HBM)] * n_in,
            out_specs=pl.BlockSpec((N_CP, PIECE, head_dim), lambda h, meta: (0, 0, h)),
            scratch_shapes=[
                pltpu.VMEM((2, seq, head_dim), jnp.bfloat16),
                pltpu.VMEM((2, seq, head_dim), jnp.bfloat16),
                pltpu.VMEM((2, N_CP, PIECE, head_dim), jnp.bfloat16),
                pltpu.VMEM((PIECE, 128), jnp.float32),
                pltpu.VMEM((PIECE, 128), jnp.float32),
                pltpu.VMEM((PIECE, head_dim), jnp.float32),
                pltpu.SemaphoreType.DMA((2,)),
            ],
        ),
        out_shape=jax.ShapeDtypeStruct((N_CP, PIECE, n_heads * head_dim), jnp.bfloat16),
        compiler_params=pltpu.CompilerParams(dimension_semantics=("arbitrary",), vmem_limit_bytes=40 * 2**20),
        cost_estimate=pl.CostEstimate(flops=30 * 10**9, bytes_accessed=30 * 2**20, transcendentals=10**7),
        name="attention",
    )(meta, starts, *k_parts, *v_parts, *q_parts)


def out_kernel(group_ref, *refs, has_recv):
    o_refs, w_refs = refs[:N_CP], refs[N_CP:2 * N_CP]
    out_ref = refs[-1]
    total = jnp.dot(o_refs[0][...], w_refs[0][...], preferred_element_type=jnp.float32)
    for src in range(1, N_CP):
        total += jnp.dot(o_refs[src][...], w_refs[src][...], preferred_element_type=jnp.float32)
    if has_recv:
        total += refs[2 * N_CP][...]
    out_ref[...] = total.astype(out_ref.dtype)


def out_proj(groups, o_parts, w_out, col0, n_cols, recv=None, y_prev=None):
    rows, width = o_parts[0].shape
    blk = 512
    first = col0 // blk
    in_specs = [pl.BlockSpec((rows, width), lambda j, g: (0, 0))] * N_CP
    in_specs += [pl.BlockSpec((width, blk), functools.partial(lambda src, j, g: (g[src], first + j), src)) for src in range(N_CP)]
    args = list(o_parts) + [w_out] * N_CP
    aliases = {}
    if recv is None:
        out_shape = jax.ShapeDtypeStruct((rows, n_cols), jnp.float32)
        out_spec = pl.BlockSpec((rows, blk), lambda j, g: (0, j))
    else:
        in_specs.append(pl.BlockSpec((rows, blk), lambda j, g: (0, j)))
        args.append(recv)
        out_shape = jax.ShapeDtypeStruct((rows, w_out.shape[1]), jnp.bfloat16)
        out_spec = pl.BlockSpec((rows, blk), lambda j, g: (0, first + j))
        if y_prev is not None:
            aliases = {1 + len(args): 0}
            in_specs.append(pl.BlockSpec(memory_space=pl.ANY))
            args.append(y_prev)
    flops = 2 * rows * width * N_CP * n_cols
    return pl.pallas_call(
        functools.partial(out_kernel, has_recv=recv is not None),
        grid_spec=pltpu.PrefetchScalarGridSpec(
            num_scalar_prefetch=1, grid=(n_cols // blk,), in_specs=in_specs, out_specs=out_spec),
        out_shape=out_shape,
        input_output_aliases=aliases,
        compiler_params=pltpu.CompilerParams(dimension_semantics=("arbitrary",), vmem_limit_bytes=40 * 2**20),
        cost_estimate=pl.CostEstimate(flops=flops, bytes_accessed=2 * width * N_CP * n_cols + 4 * rows * n_cols, transcendentals=0),
        name="out_proj",
    )(groups, *args)


def solution(mesh):
    def per_device(x_loc, seg_loc, w_q, w_k, w_v, w_o):
        cp_rank = lax.axis_index("cp")
        tp_rank = lax.axis_index("tp")
        rows = x_loc.shape[0]
        n_loc, head_dim = w_k.shape[1:]
        n_grp = n_loc // N_CP
        coef = head_dim ** -0.5 * math.log2(math.e)
        half = rows // X_CHUNKS

        x_other = []
        for c in range(X_CHUNKS):
            x_other.append(lax.ppermute(x_loc[c * half:(c + 1) * half], "tp", SWAP))

        seg_all = lax.all_gather(seg_loc, ("cp", "tp"), axis=0, tiled=True).reshape(N_CP, 2, PIECE)
        seg_pos = jnp.concatenate([seg_all[:, 0], seg_all[::-1, 1]], axis=0).reshape(-1)
        seq = seg_pos.shape[0]
        n_blk = seq // PIECE
        starts = jnp.sum((seg_pos[None, :] < seg_pos[:, None]).astype(jnp.int32), axis=1)
        blk_starts = starts.reshape(n_blk, PIECE)
        k_lo = blk_starts[:, 0] // PIECE
        k_full = jnp.minimum((blk_starts[:, -1] + PIECE - 1) // PIECE, jnp.arange(n_blk))
        ranks = jnp.array([cp_rank ^ s for s in range(N_CP)])
        own_piece = jnp.where(tp_rank == 0, ranks, 2 * N_CP - 1 - ranks)
        other_piece = 2 * N_CP - 1 - own_piece

        def meta_of(q_piece):
            return jnp.concatenate([own_piece, other_piece, q_piece, k_lo, k_full]).astype(jnp.int32)

        def project(x_rows, w):
            out = jnp.einsum("sd,dhe->she", x_rows, w, preferred_element_type=jnp.float32).astype(jnp.bfloat16)
            return out.transpose(1, 0, 2)

        def slices(val):
            return [lax.dynamic_slice_in_dim(val, (cp_rank ^ s) * n_grp, n_grp, axis=0) for s in range(N_CP)]

        def exchange(parts):
            out = [parts[0]] + [None] * (N_CP - 1)
            for s in (2, 3, 1):
                out[s] = lax.ppermute(parts[s], "cp", [(d, d ^ s) for d in range(N_CP)])
            return out

        weights = (w_k, w_v, w_q)
        inputs = [x_loc] + x_other
        spread = []
        held = None
        for c, x_c in enumerate(inputs):
            done = []
            for i, w in enumerate(weights):
                if held is not None:
                    x_c, held = lax.optimization_barrier((x_c, held))
                    if c != 1 or i != 0:
                        (done if i else spread[-1]).append(exchange(held))
                val = project(x_c, w)
                held = slices(val)
                if c == 0 and i == 2:
                    q_own = held
            spread.append(done)
        spread[-1].append(exchange(held))
        ks, vs = [d[0] for d in spread], [d[1] for d in spread]
        qs = [d[2] for d in spread[1:]]

        chunk_rows = [(0, 0, rows)] + [(1, c * half, half) for c in range(X_CHUNKS)]
        k_parts = [ks[i][s] for s in range(N_CP) for i in range(1 + X_CHUNKS)]
        v_parts = [vs[i][s] for s in range(N_CP) for i in range(1 + X_CHUNKS)]
        starts_col = starts[:, None]
        o_other = attention(meta_of(other_piece), starts_col, k_parts, v_parts,
                            [qs[c][s] for s in range(N_CP) for c in range(X_CHUNKS)],
                            chunk_rows, [(c * half, half) for c in range(X_CHUNKS)], coef)

        w_out = w_o.reshape(n_loc * head_dim, -1)
        groups = ranks.astype(jnp.int32)
        back_other = exchange([o_other[s] for s in range(N_CP)])
        q_own, back_other = lax.optimization_barrier((q_own, back_other))
        qs_own = exchange(q_own)
        recvs = []
        part = None
        col0 = 0
        for n_cols in Y_SPLITS:
            if part is not None:
                groups, part = lax.optimization_barrier((groups, part))
                recvs.append(lax.ppermute(part, "tp", SWAP))
            part = out_proj(groups, back_other, w_out, col0, n_cols)
            col0 += n_cols
        meta_own, part = lax.optimization_barrier((meta_of(own_piece), part))
        recvs.append(lax.ppermute(part, "tp", SWAP))
        o_own = attention(meta_own, starts_col, k_parts, v_parts,
                          [qs_own[s] for s in range(N_CP)], chunk_rows, [(0, rows)], coef)
        back_own = exchange([o_own[s] for s in range(N_CP)])
        y = None
        col0 = 0
        for n_cols, recv in zip(Y_SPLITS, recvs):
            y = out_proj(groups, back_own, w_out, col0, n_cols, recv, y)
            col0 += n_cols
        return y

    return jax.shard_map(
        per_device,
        mesh=mesh,
        in_specs=(P(("dp", "cp", "tp"), None), P(("dp", "cp", "tp")), P(None, "tp", None), P(None, "tp", None), P(None, "tp", None), P("tp", None, None)),
        out_specs=P(("dp", "cp", "tp"), None),
        check_vma=False,
    )
```

```python
import functools
import math

import jax
import jax.numpy as jnp
from jax import lax
from jax.experimental import pallas as pl
from jax.experimental.pallas import tpu as pltpu
from jax.sharding import PartitionSpec as P


NEG_BIG = -1e30
N_CP = 4
PIECE = 512
PAIR = 2
HALVES = 2
X_CHUNKS = 2
Y_SPLITS = (512, 1024, 1024, 1024, 1024, 1024, 1024, 1024, 512)
SWAP = [(0, 1), (1, 0)]


def attn_kernel(meta_ref, start_ref, *refs, head0, n_steps, k_chunks, q_chunks, coef):
    n_parts = len(k_chunks)
    n_k = N_CP * n_parts
    n_q = N_CP * len(q_chunks)
    k_refs, v_refs = refs[:n_k], refs[n_k:2 * n_k]
    q_refs = refs[2 * n_k:2 * n_k + n_q]
    o_ref = refs[2 * n_k + n_q]
    k_buf, v_buf, q_buf, acc_ref, sems = refs[2 * n_k + n_q + 1:]
    step_idx = pl.program_id(0)

    def copies(idx, slot):
        heads = pl.ds(head0 + idx * PAIR, PAIR)
        out = []
        for src in range(N_CP):
            for part, (kind, row0, rows) in enumerate(k_chunks):
                piece = meta_ref[kind * N_CP + src]
                dst = pl.ds(pl.multiple_of(piece * PIECE + row0, 128), rows)
                i = src * n_parts + part
                out.append(pltpu.make_async_copy(k_refs[i].at[heads], k_buf.at[slot, :, dst], sems.at[slot]))
                out.append(pltpu.make_async_copy(v_refs[i].at[heads], v_buf.at[slot, :, dst], sems.at[slot]))
            for part, (row0, rows) in enumerate(q_chunks):
                i = src * len(q_chunks) + part
                out.append(pltpu.make_async_copy(q_refs[i].at[heads], q_buf.at[slot, :, src, pl.ds(row0, rows)], sems.at[slot]))
        return out

    slot = lax.rem(step_idx, 2)

    @pl.when(step_idx == 0)
    def _():
        for cp in copies(0, 0):
            cp.start()

    @pl.when(step_idx + 1 < n_steps)
    def _():
        for cp in copies(step_idx + 1, 1 - slot):
            cp.start()

    for cp in copies(step_idx, slot):
        cp.wait()

    key_i = lax.broadcasted_iota(jnp.int32, (PIECE, PIECE), 0)
    qry_i = lax.broadcasted_iota(jnp.int32, (PIECE, PIECE), 1)

    for src in range(N_CP):
        q_piece = meta_ref[2 * N_CP + src]
        k_lo = meta_ref[3 * N_CP + src]
        k_full = meta_ref[4 * N_CP + src]
        q0 = pl.multiple_of(q_piece * PIECE, PIECE)
        starts = start_ref[src]

        def scores_of(h, k0):
            return lax.dot_general(k_buf[slot, h, pl.ds(k0, PIECE), :], q_buf[slot, h, src], (((1,), (1,)), ((), ())), preferred_element_type=jnp.float32)

        def weighted(h, k0, p):
            return lax.dot_general(v_buf[slot, h, pl.ds(k0, PIECE), :], p.astype(jnp.bfloat16), (((0,), (0,)), ((), ())), preferred_element_type=jnp.float32)

        state = []
        for h in range(PAIR):
            s = scores_of(h, q0)
            s = jnp.where((key_i <= qry_i) & (key_i >= starts - q0), s, NEG_BIG)
            m_new = jnp.max(s, axis=0, keepdims=True)
            p = jnp.exp2(s * coef - m_new * coef)
            acc_ref[h] = weighted(h, q0, p)
            state.append((m_new, jnp.sum(p, axis=0, keepdims=True)))

        def step(kb, state, masked):
            k0 = pl.multiple_of(kb * PIECE, PIECE)
            out = []
            for h in range(PAIR):
                m_old, l_old = state[h]
                s = scores_of(h, k0)
                if masked:
                    s = jnp.where(key_i >= starts - k0, s, NEG_BIG)
                m_new = jnp.maximum(m_old, jnp.max(s, axis=0, keepdims=True))
                alpha = jnp.exp2((m_old - m_new) * coef)
                p = jnp.exp2(s * coef - m_new * coef)
                acc_ref[h] = acc_ref[h] * alpha + weighted(h, k0, p)
                out.append((m_new, l_old * alpha + jnp.sum(p, axis=0, keepdims=True)))
            return tuple(out)

        state = lax.fori_loop(k_lo, k_full, functools.partial(step, masked=True), tuple(state))
        state = lax.fori_loop(k_full, q_piece, functools.partial(step, masked=False), state)
        for h in range(PAIR):
            out = acc_ref[h] / state[h][1]
            o_ref[src, :, h * 128:(h + 1) * 128] = out.T.astype(jnp.bfloat16)


def attention(meta, starts, k_parts, v_parts, q_parts, k_chunks, q_chunks, coef, head0, n_heads):
    head_dim = k_parts[0].shape[-1]
    n_in = len(k_parts) + len(v_parts) + len(q_parts)
    seq = 2 * N_CP * PIECE
    n_steps = n_heads // PAIR
    return pl.pallas_call(
        functools.partial(attn_kernel, head0=head0, n_steps=n_steps, k_chunks=k_chunks, q_chunks=q_chunks, coef=coef),
        grid_spec=pltpu.PrefetchScalarGridSpec(
            num_scalar_prefetch=1,
            grid=(n_steps,),
            in_specs=[pl.BlockSpec((N_CP, 1, PIECE), lambda h, meta: (0, 0, 0))] + [pl.BlockSpec(memory_space=pltpu.HBM)] * n_in,
            out_specs=pl.BlockSpec((N_CP, PIECE, PAIR * head_dim), lambda h, meta: (0, 0, h)),
            scratch_shapes=[
                pltpu.VMEM((2, PAIR, seq, head_dim), jnp.bfloat16),
                pltpu.VMEM((2, PAIR, seq, head_dim), jnp.bfloat16),
                pltpu.VMEM((2, PAIR, N_CP, PIECE, head_dim), jnp.bfloat16),
                pltpu.VMEM((PAIR, head_dim, PIECE), jnp.float32),
                pltpu.SemaphoreType.DMA((2,)),
            ],
        ),
        out_shape=jax.ShapeDtypeStruct((N_CP, PIECE, n_heads * head_dim), jnp.bfloat16),
        compiler_params=pltpu.CompilerParams(dimension_semantics=("arbitrary",), vmem_limit_bytes=48 * 2**20),
        cost_estimate=pl.CostEstimate(flops=15 * 10**9, bytes_accessed=15 * 2**20, transcendentals=10**7),
        name="attention",
    )(meta, starts, *k_parts, *v_parts, *q_parts)


def out_kernel(group_ref, *refs, n_parts, has_recv):
    o_refs, w_refs = refs[:n_parts], refs[n_parts:2 * n_parts]
    out_ref = refs[-1]
    total = jnp.dot(o_refs[0][...], w_refs[0][...], preferred_element_type=jnp.float32)
    for src in range(1, n_parts):
        total += jnp.dot(o_refs[src][...], w_refs[src][...], preferred_element_type=jnp.float32)
    if has_recv:
        total += refs[2 * n_parts][...]
    out_ref[...] = total.astype(out_ref.dtype)


def out_proj(groups, o_parts, w_out, col0, n_cols, recv=None, y_prev=None):
    rows, width = o_parts[0].shape
    n_parts = len(o_parts)
    blk = 512
    first = col0 // blk
    in_specs = [pl.BlockSpec((rows, width), lambda j, g: (0, 0))] * n_parts
    in_specs += [pl.BlockSpec((width, blk), functools.partial(lambda src, j, g: (g[src], first + j), src)) for src in range(n_parts)]
    args = list(o_parts) + [w_out] * n_parts
    aliases = {}
    if recv is None:
        out_shape = jax.ShapeDtypeStruct((rows, n_cols), jnp.float32)
        out_spec = pl.BlockSpec((rows, blk), lambda j, g: (0, j))
    else:
        in_specs.append(pl.BlockSpec((rows, blk), lambda j, g: (0, j)))
        args.append(recv)
        out_shape = jax.ShapeDtypeStruct((rows, w_out.shape[1]), jnp.bfloat16)
        out_spec = pl.BlockSpec((rows, blk), lambda j, g: (0, first + j))
        if y_prev is not None:
            aliases = {1 + len(args): 0}
            in_specs.append(pl.BlockSpec(memory_space=pl.ANY))
            args.append(y_prev)
    flops = 2 * rows * width * n_parts * n_cols
    return pl.pallas_call(
        functools.partial(out_kernel, n_parts=n_parts, has_recv=recv is not None),
        grid_spec=pltpu.PrefetchScalarGridSpec(
            num_scalar_prefetch=1, grid=(n_cols // blk,), in_specs=in_specs, out_specs=out_spec),
        out_shape=out_shape,
        input_output_aliases=aliases,
        compiler_params=pltpu.CompilerParams(dimension_semantics=("arbitrary",), vmem_limit_bytes=40 * 2**20),
        cost_estimate=pl.CostEstimate(flops=flops, bytes_accessed=2 * width * n_parts * n_cols + 4 * rows * n_cols, transcendentals=0),
        name="out_proj",
    )(groups, *args)


def solution(mesh):
    def per_device(x_loc, seg_loc, w_q, w_k, w_v, w_o):
        cp_rank = lax.axis_index("cp")
        tp_rank = lax.axis_index("tp")
        rows = x_loc.shape[0]
        n_loc, head_dim = w_k.shape[1:]
        n_grp = n_loc // N_CP
        coef = head_dim ** -0.5 * math.log2(math.e)
        half = rows // X_CHUNKS

        def cp_perm(s):
            return [(d, d ^ s) for d in range(N_CP)]

        seg_pair = jnp.stack([seg_loc, lax.ppermute(seg_loc, "tp", SWAP)])
        x_other = []
        for c in range(X_CHUNKS):
            x_other.append(lax.ppermute(x_loc[c * half:(c + 1) * half], "tp", SWAP))

        def project(x_rows, w):
            out = jnp.einsum("sd,dhe->she", x_rows, w, preferred_element_type=jnp.float32).astype(jnp.bfloat16)
            return out.transpose(1, 0, 2)

        def slices(val):
            return [lax.dynamic_slice_in_dim(val, (cp_rank ^ s) * n_grp, n_grp, axis=0) for s in range(N_CP)]

        def exchange(parts):
            out = [parts[0]] + [None] * (N_CP - 1)
            for s in (2, 3, 1):
                out[s] = lax.ppermute(parts[s], "cp", cp_perm(s))
            return out

        jobs = [(x_loc, w_k, False), (x_loc, w_v, False)]
        for c in range(X_CHUNKS):
            jobs += [(x_other[c], w, w is w_k) for w in (w_k, w_v, w_q)]
        spread = []
        held = x_c = None
        for i, (x_new, w, fresh) in enumerate(jobs):
            x_c = x_new if i == 0 or fresh else x_c
            if held is not None:
                x_c, held = lax.optimization_barrier((x_c, held))
                spread.append(exchange(held))
            val = project(x_c, w)
            held = slices(val)
        spread.append(exchange(held))
        ks = [spread[0]] + spread[2::3]
        vs = [spread[1]] + spread[3::3]
        qs = spread[4::3]

        seg_all = jnp.stack([seg_pair] + [lax.ppermute(seg_pair, "cp", cp_perm(s)) for s in range(1, N_CP)])
        starts = jnp.sum((seg_all.reshape(1, -1) < seg_all.reshape(-1, 1)).astype(jnp.int32), axis=1).reshape(N_CP, 2, rows)
        ranks = jnp.array([cp_rank ^ s for s in range(N_CP)])
        own_piece = jnp.where(tp_rank == 0, ranks, 2 * N_CP - 1 - ranks)
        other_piece = 2 * N_CP - 1 - own_piece

        def meta_of(kind, q_piece):
            first, last = starts[:, kind, 0], starts[:, kind, -1]
            k_full = jnp.minimum((last + PIECE - 1) // PIECE, q_piece)
            return jnp.concatenate([own_piece, other_piece, q_piece, first // PIECE, k_full]).astype(jnp.int32)

        k_chunks = [(0, 0, rows)] + [(1, c * half, half) for c in range(X_CHUNKS)]
        k_parts = [k[s] for s in range(N_CP) for k in ks]
        v_parts = [v[s] for s in range(N_CP) for v in vs]
        n_half = n_grp // HALVES
        meta_other = meta_of(1, other_piece)
        starts_other = starts[:, 1][:, None]
        q_parts = [q[s] for s in range(N_CP) for q in qs]
        back_other = [None] * (N_CP * HALVES)
        for hf in range(HALVES):
            o_half = attention(meta_other, starts_other, k_parts, v_parts, q_parts, k_chunks,
                               [(c * half, half) for c in range(X_CHUNKS)], coef, hf * n_half, n_half)
            o_slots = [o_half[s] for s in range(N_CP)]
            if hf + 1 < HALVES:
                meta_other, o_slots = lax.optimization_barrier((meta_other, o_slots))
            back_other[hf::HALVES] = exchange(o_slots)

        w_out = w_o.reshape(n_loc * head_dim, -1)
        groups = jnp.stack([ranks * HALVES + hf for hf in range(HALVES)], axis=1).reshape(-1).astype(jnp.int32)
        recvs = []
        part = None
        col0 = 0
        for n_cols in Y_SPLITS:
            if part is not None:
                groups, part = lax.optimization_barrier((groups, part))
                recvs.append(lax.ppermute(part, "tp", SWAP))
            part = out_proj(groups, back_other, w_out, col0, n_cols)
            col0 += n_cols
        x_own, part = lax.optimization_barrier((x_loc, part))
        recvs.append(lax.ppermute(part, "tp", SWAP))
        q_own = project(x_own, w_q)
        qs_own = exchange(slices(q_own))
        o_own = attention(meta_of(0, own_piece), starts[:, 0][:, None], k_parts, v_parts,
                          qs_own, k_chunks, [(0, rows)], coef, 0, n_grp)
        back_own = exchange([o_own[s] for s in range(N_CP)])
        own_groups = ranks.astype(jnp.int32)
        y = None
        col0 = 0
        for n_cols, recv in zip(Y_SPLITS, recvs):
            y = out_proj(own_groups, back_own, w_out, col0, n_cols, recv, y)
            col0 += n_cols
        return y

    return jax.shard_map(
        per_device,
        mesh=mesh,
        in_specs=(P(("dp", "cp", "tp"), None), P(("dp", "cp", "tp")), P(None, "tp", None), P(None, "tp", None), P(None, "tp", None), P("tp", None, None)),
        out_specs=P(("dp", "cp", "tp"), None),
        check_vma=False,
    )
```

```python
import functools
import math

import jax
import jax.numpy as jnp
from jax import lax
from jax.experimental import pallas as pl
from jax.experimental.pallas import tpu as pltpu
from jax.sharding import PartitionSpec as P


NEG_BIG = -1e30
N_CP = 4
N_DOCS = 6
PIECE = 512
HALF = 256
KEYS = 512
PAD = KEYS - HALF
PAIR = 4
Y_SPLITS = (1024, 3072, 3072, 512, 512)
SWAP = [(0, 1), (1, 0)]


def attn_kernel(meta_ref, start_ref, *refs, head0, n_steps, k_chunks, q_row0, coef):
    n_parts = len(k_chunks)
    n_k = N_CP * n_parts
    k_refs, v_refs, q_refs = refs[:n_k], refs[n_k:2 * n_k], refs[2 * n_k:2 * n_k + N_CP]
    o_ref, k_buf, v_buf, q_buf, acc_ref, sems = refs[2 * n_k + N_CP:]
    step_idx = pl.program_id(0)

    def copies(idx, slot):
        heads = pl.ds(head0 + idx * PAIR, PAIR)
        out = []
        for src in range(N_CP):
            for part, (kind, row0, rows) in enumerate(k_chunks):
                piece = meta_ref[kind * N_CP + src]
                dst = pl.ds(pl.multiple_of(piece * PIECE + row0 + PAD, 128), rows)
                i = src * n_parts + part
                out.append(pltpu.make_async_copy(k_refs[i].at[heads], k_buf.at[slot, :, dst], sems.at[slot]))
                out.append(pltpu.make_async_copy(v_refs[i].at[heads], v_buf.at[slot, :, dst], sems.at[slot]))
            out.append(pltpu.make_async_copy(q_refs[src].at[heads, pl.ds(q_row0, HALF)], q_buf.at[slot, :, src], sems.at[slot]))
        return out

    slot = lax.rem(step_idx, 2)

    @pl.when(step_idx == 0)
    def _():
        for cp in copies(0, 0):
            cp.start()
        for buf in (k_buf, v_buf):
            for which in range(2):
                for h in range(PAIR):
                    buf[which, h, :PAD, :] = jnp.zeros((PAD, buf.shape[-1]), buf.dtype)

    @pl.when(step_idx + 1 < n_steps)
    def _():
        for cp in copies(step_idx + 1, 1 - slot):
            cp.start()

    for cp in copies(step_idx, slot):
        cp.wait()

    def scores_of(h, src, row, n):
        return lax.dot_general(k_buf[slot, h, pl.ds(row, n), :], q_buf[slot, h, src], (((1,), (1,)), ((), ())), preferred_element_type=jnp.float32)

    def weighted(h, row, n, p):
        return lax.dot_general(v_buf[slot, h, pl.ds(row, n), :], p.astype(jnp.bfloat16), (((0,), (0,)), ((), ())), preferred_element_type=jnp.float32)

    def one_piece(src, carry):
        q0 = pl.multiple_of(meta_ref[2 * N_CP + src], HALF)
        n_full = meta_ref[3 * N_CP + src]
        n_all = meta_ref[4 * N_CP + src]
        starts = start_ref[src]
        row = pl.multiple_of(q0 + PAD, HALF)
        key_d = lax.broadcasted_iota(jnp.int32, (HALF, HALF), 0)
        qry_d = lax.broadcasted_iota(jnp.int32, (HALF, HALF), 1)
        key_i = lax.broadcasted_iota(jnp.int32, (KEYS, HALF), 0)
        scores = [scores_of(h, src, row, HALF) for h in range(PAIR)]
        state = []
        for h in range(PAIR):
            s = jnp.where((key_d <= qry_d) & (key_d >= starts - q0), scores[h], NEG_BIG)
            m_new = jnp.max(s, axis=0, keepdims=True)
            p = jnp.exp2(s * coef - m_new * coef)
            acc_ref[h] = weighted(h, row, HALF, p)
            state.append((m_new, jnp.sum(p, axis=0, keepdims=True)))

        def step(j, state, masked):
            row = pl.multiple_of(q0 + PAD - (j + 1) * KEYS, HALF)
            scores = [scores_of(h, src, row, KEYS) for h in range(PAIR)]
            out = []
            for h in range(PAIR):
                m_old, l_old = state[h]
                s = scores[h]
                if masked:
                    s = jnp.where(key_i >= starts + (PAD - row), s, NEG_BIG)
                m_new = jnp.maximum(m_old, jnp.max(s, axis=0, keepdims=True))
                alpha = jnp.exp2((m_old - m_new) * coef)
                p = jnp.exp2(s * coef - m_new * coef)
                acc_ref[h] = acc_ref[h] * alpha + weighted(h, row, KEYS, p)
                out.append((m_new, l_old * alpha + jnp.sum(p, axis=0, keepdims=True)))
            return tuple(out)

        state = lax.fori_loop(0, n_full, functools.partial(step, masked=False), tuple(state))
        state = lax.fori_loop(n_full, n_all, functools.partial(step, masked=True), state)
        for h in range(PAIR):
            out = acc_ref[h] / state[h][1]
            o_ref[src, :, h * 128:(h + 1) * 128] = out.T.astype(jnp.bfloat16)
        return carry

    lax.fori_loop(0, N_CP, one_piece, 0)


def attention(meta, starts, k_parts, v_parts, q_parts, k_chunks, q_row0, coef, head0, n_heads):
    head_dim = k_parts[0].shape[-1]
    n_in = len(k_parts) + len(v_parts) + len(q_parts)
    seq = 2 * N_CP * PIECE
    n_steps = n_heads // PAIR
    return pl.pallas_call(
        functools.partial(attn_kernel, head0=head0, n_steps=n_steps, k_chunks=k_chunks, q_row0=q_row0, coef=coef),
        grid_spec=pltpu.PrefetchScalarGridSpec(
            num_scalar_prefetch=1,
            grid=(n_steps,),
            in_specs=[pl.BlockSpec((N_CP, 1, HALF), lambda h, meta: (0, 0, 0))] + [pl.BlockSpec(memory_space=pltpu.HBM)] * n_in,
            out_specs=pl.BlockSpec((N_CP, HALF, PAIR * head_dim), lambda h, meta: (0, 0, h)),
            scratch_shapes=[
                pltpu.VMEM((2, PAIR, seq + PAD, head_dim), jnp.bfloat16),
                pltpu.VMEM((2, PAIR, seq + PAD, head_dim), jnp.bfloat16),
                pltpu.VMEM((2, PAIR, N_CP, HALF, head_dim), jnp.bfloat16),
                pltpu.VMEM((PAIR, head_dim, HALF), jnp.float32),
                pltpu.SemaphoreType.DMA((2,)),
            ],
        ),
        out_shape=jax.ShapeDtypeStruct((N_CP, HALF, n_heads * head_dim), jnp.bfloat16),
        compiler_params=pltpu.CompilerParams(dimension_semantics=("arbitrary",), vmem_limit_bytes=44 * 2**20),
        cost_estimate=pl.CostEstimate(flops=15 * 10**9, bytes_accessed=15 * 2**20, transcendentals=10**7),
        name="attention",
    )(meta, starts, *k_parts, *v_parts, *q_parts)


def out_kernel(group_ref, *refs, n_parts, n_recv):
    o_refs, w_ref = refs[:n_parts], refs[n_parts]
    out_ref, o_buf = refs[-2:]
    width = o_refs[0].shape[1]

    @pl.when(pl.program_id(0) == 0)
    def _():
        for src in range(n_parts):
            o_buf[:, pl.ds(pl.multiple_of(group_ref[src] * width, 128), width)] = o_refs[src][...]

    total = jnp.dot(o_buf[...], w_ref[...], preferred_element_type=jnp.float32)
    if n_recv == 0:
        out_ref[...] = total
    for i in range(n_recv):
        at = slice(i * HALF, (i + 1) * HALF)
        out_ref[at] = (total[at] + refs[n_parts + 1 + i][...]).astype(out_ref.dtype)


def out_proj(groups, o_parts, w_out, col0, n_cols, recvs=(), y_prev=None):
    rows, width = o_parts[0].shape
    n_parts = len(o_parts)
    depth, all_cols = w_out.shape
    blk = 1024 if n_cols % 1024 == 0 and col0 % 1024 == 0 else 512
    first = col0 // blk
    in_specs = [pl.BlockSpec((rows, width), lambda j, g: (0, 0))] * n_parts
    in_specs.append(pl.BlockSpec((depth, blk), lambda j, g: (0, first + j)))
    in_specs += [pl.BlockSpec((HALF, blk), lambda j, g: (0, j))] * len(recvs)
    args = [*o_parts, w_out, *recvs]
    aliases = {}
    if recvs:
        out_shape = jax.ShapeDtypeStruct((rows, all_cols), jnp.bfloat16)
        out_spec = pl.BlockSpec((rows, blk), lambda j, g: (0, first + j))
        if y_prev is not None:
            aliases = {1 + len(args): 0}
            in_specs.append(pl.BlockSpec(memory_space=pl.ANY))
            args.append(y_prev)
    else:
        out_shape = jax.ShapeDtypeStruct((rows, n_cols), jnp.float32)
        out_spec = pl.BlockSpec((rows, blk), lambda j, g: (0, j))
    return pl.pallas_call(
        functools.partial(out_kernel, n_parts=n_parts, n_recv=len(recvs)),
        grid_spec=pltpu.PrefetchScalarGridSpec(
            num_scalar_prefetch=1, grid=(n_cols // blk,), in_specs=in_specs, out_specs=out_spec,
            scratch_shapes=[pltpu.VMEM((rows, depth), jnp.bfloat16)]),
        out_shape=out_shape,
        input_output_aliases=aliases,
        compiler_params=pltpu.CompilerParams(dimension_semantics=("arbitrary",), vmem_limit_bytes=40 * 2**20),
        cost_estimate=pl.CostEstimate(flops=2 * rows * depth * n_cols, bytes_accessed=2 * depth * n_cols + 4 * rows * n_cols, transcendentals=0),
        name="out_proj",
    )(groups, *args)


def solution(mesh):
    def per_device(x_loc, seg_loc, w_q, w_k, w_v, w_o):
        cp_rank = lax.axis_index("cp")
        tp_rank = lax.axis_index("tp")
        rows = x_loc.shape[0]
        n_loc, head_dim = w_k.shape[1:]
        n_grp = n_loc // N_CP
        coef = head_dim ** -0.5 * math.log2(math.e)

        def cp_perm(s):
            return [(d, d ^ s) for d in range(N_CP)]

        def swap(val):
            return lax.ppermute(val, "tp", SWAP)

        def project(x_rows, w):
            out = jnp.einsum("sd,dhe->she", x_rows, w, preferred_element_type=jnp.float32).astype(jnp.bfloat16)
            return out.transpose(1, 0, 2)

        def slices(val):
            return [lax.dynamic_slice_in_dim(val, (cp_rank ^ s) * n_grp, n_grp, axis=0) for s in range(N_CP)]

        def exchange(parts):
            out = [parts[0]] + [None] * (N_CP - 1)
            for s in (2, 3, 1):
                out[s] = lax.ppermute(parts[s], "cp", cp_perm(s))
            return out

        def after(val, other):
            return lax.optimization_barrier((val, other))

        seg_pair = jnp.stack([seg_loc, swap(seg_loc)])
        x_a = swap(x_loc[:HALF])
        k_own = slices(project(x_loc, w_k))
        x_late, k_own = after(x_loc, k_own)
        x_b = swap(x_late[HALF:])
        x_cur = x_late
        ks = [exchange(k_own)]
        held = slices(project(x_cur, w_v))

        seg_all = jnp.stack([seg_pair] + [lax.ppermute(seg_pair, "cp", cp_perm(s)) for s in range(1, N_CP)])
        ids = jnp.arange(N_DOCS, dtype=jnp.int32)[:, None, None, None]
        counts = jnp.sum((seg_all[None] == ids).astype(jnp.int32), axis=(1, 2, 3), keepdims=True)
        starts = jnp.sum(jnp.where(ids < seg_all[None], counts, 0), axis=0)
        ranks = jnp.array([cp_rank ^ s for s in range(N_CP)])
        own_piece = jnp.where(tp_rank == 0, ranks, 2 * N_CP - 1 - ranks)
        other_piece = 2 * N_CP - 1 - own_piece
        metas = []
        for kind, piece in enumerate((own_piece, other_piece)):
            for hf in range(2):
                q0 = piece * PIECE + hf * HALF
                first, last = starts[:, kind, hf * HALF], starts[:, kind, (hf + 1) * HALF - 1]
                n_full = jnp.maximum(q0 - last, 0) // KEYS
                n_all = jnp.maximum(q0 - first + KEYS - 1, 0) // KEYS
                meta = jnp.concatenate([own_piece, other_piece, q0, n_full, n_all]).astype(jnp.int32)
                metas.append((meta, starts[:, kind, hf * HALF:(hf + 1) * HALF][:, None]))

        x_cur, held = after(x_a, held)
        vs = [exchange(held)]
        for i, (x_new, w) in enumerate(((x_cur, w_k), (None, w_v), (None, w_q), (x_b, w_k), (None, w_v), (None, w_q))):
            if i:
                x_cur, held = after(x_cur if x_new is None else x_new, held)
                (ks, vs, qs)[(i - 1) % 3].append(exchange(held))
                if i == 2:
                    x_cur, metas = after(x_cur, metas)
            else:
                qs = []
            held = slices(project(x_cur, w))
        metas, held = after(metas, held)
        qs.append(exchange(held))

        k_chunks = [(0, 0, rows), (1, 0, HALF), (1, HALF, HALF)]
        k_parts = [k[s] for s in range(N_CP) for k in ks]
        v_parts = [v[s] for s in range(N_CP) for v in vs]

        def attend(which, q_parts, q_row0, head0=0, n_heads=n_grp):
            o_all = attention(*which, k_parts, v_parts, q_parts, k_chunks, q_row0, coef, head0, n_heads)
            return [o_all[s] for s in range(N_CP)]

        w_out = w_o.reshape(n_loc * head_dim, -1)
        whole = ranks.astype(jnp.int32)
        halves = jnp.stack([ranks * 2, ranks * 2 + 1], axis=1).reshape(-1).astype(jnp.int32)

        def partials(groups, o_parts):
            recvs, part, col0 = [], None, 0
            for n_cols in Y_SPLITS:
                if part is not None:
                    groups, part = after(groups, part)
                    recvs.append(swap(part))
                part = out_proj(groups, o_parts, w_out, col0, n_cols)
                col0 += n_cols
            return recvs, part

        n_half = n_grp // 2
        o_a0 = attend(metas[2], qs[0], 0, 0, n_half)
        meta_a1, o_a0 = after(metas[2], o_a0)
        back_a0 = exchange(o_a0)
        o_a1 = attend(meta_a1, qs[0], 0, n_half, n_half)
        back_a1 = exchange(o_a1)
        back_a = [b[s] for s in range(N_CP) for b in (back_a0, back_a1)]
        recv_a, part = partials(halves, back_a)
        x_cur, part = after(x_loc, part)
        recv_a.append(swap(part))
        q_own = slices(project(x_cur, w_q))
        meta_b, q_own = after(metas[3], q_own)
        q_own = exchange(q_own)
        o_b = attend(meta_b, qs[1], 0)
        meta_oa, o_b = after(metas[0], o_b)
        back_b = exchange(o_b)
        o_oa = attend(meta_oa, q_own, 0)
        groups_b, o_oa = after(whole, o_oa)
        recv_b, part = partials(groups_b, back_b)
        meta_ob, part = after(metas[1], part)
        recv_b.append(swap(part))
        o_ob = attend(meta_ob, q_own, HALF)
        back_own = exchange([jnp.concatenate(pair, axis=0) for pair in zip(o_oa, o_ob)])
        y = None
        col0 = 0
        for i, n_cols in enumerate(Y_SPLITS):
            y = out_proj(whole, back_own, w_out, col0, n_cols, (recv_a[i], recv_b[i]), y)
            col0 += n_cols
        return y

    return jax.shard_map(
        per_device,
        mesh=mesh,
        in_specs=(P(("dp", "cp", "tp"), None), P(("dp", "cp", "tp")), P(None, "tp", None), P(None, "tp", None), P(None, "tp", None), P("tp", None, None)),
        out_specs=P(("dp", "cp", "tp"), None),
        check_vma=False,
    )
```
